32 devices in a mesh: win: 8 (over z, x), band: 4 (over y, core).
Axes of the slice: x: 2, y: 2, z: 4, core: 2. Of those that a mesh axis runs over, the one named last changes fastest.
Arguments:
- vis: bfloat16 [32768, 2, 1024], P(('win', 'band')), may hold values from -6 to 6
- inv_noise: float32 [32768, 1024], P(('win', 'band')), may hold values from 0.14 to 4.2
- assign: int32 [32768], P(('win', 'band')), may hold values from 0 to 63, as said below
- taper_bank: float32 [4, 1024], replicated, may hold values from 0.2 to 1.25
- taper_pick: int32 [32], replicated, may hold values from 0 to 3
Outputs:
- window_fn: float32 [32, 512, 512], P(('win', 'band'))
The draws below stay inside these ranges and needn't reach their ends.
Inputs may be any that keep to these rules, and one draw needn't show every extreme that they name: `assign`: in the rows of one device no value is named by more than 32 pairs; one value is named by exactly 32 pairs in the rows of every device.
All inputs are finite; a program needn't handle non-finite values.
Results may differ from the reference program's by a relative error of at most 0.0014.
Values may be sent and summed in bfloat16 or wider, within the bound.
No kernel may reach another device: no remote copies, remote signals or barrier semaphores. Data moves between devices by JAX's collectives and lax.ppermute only.
A program may use at most 64 MiB of HBM per device.

```python
import math
import jax
import jax.numpy as jnp
from jax import lax

FREQ = 1024
P_SIZE = 512
TAPERS = 4
PAIR_DEV = 1024
WINDOWS = 32
CAP = 32
PAIRS = 32768


def assign_table(key):
    devices = PAIRS // PAIR_DEV
    group_lanes = 2 * WINDOWS
    base_key = jax.random.fold_in(key, 7)
    full_ident = jax.random.randint(jax.random.fold_in(base_key, 5), (), 0, group_lanes, dtype=jnp.int32)

    def one_device(index):
        device_key = jax.random.fold_in(base_key, 100 + index)
        slot_pool = jax.random.permutation(jax.random.fold_in(device_key, 1), (group_lanes - 1) * CAP)
        others = (slot_pool[:PAIR_DEV - CAP] // CAP).astype(jnp.int32)
        others = others + (others >= full_ident).astype(jnp.int32)
        device_ids = jnp.concatenate([jnp.full((CAP,), full_ident, jnp.int32), others])
        shuffle = jax.random.permutation(jax.random.fold_in(device_key, 2), PAIR_DEV)
        return device_ids[shuffle]
    return jax.vmap(one_device)(jnp.arange(devices, dtype=jnp.int32)).reshape(PAIRS)


def draw_assign(key, part):
    return assign_table(key)


def draw_inv_noise(key, part):
    scale_key = jax.random.fold_in(key, 43)
    rough_key = jax.random.fold_in(key, 47)
    window_pos = ((assign_table(key) // 2).astype(jnp.float32) / max(WINDOWS - 1, 1))[:, None]
    rising = 0.8 + 0.4 * window_pos
    scales = jnp.exp(jax.random.uniform(scale_key, (PAIRS, 1), jnp.float32, math.log(0.3), math.log(2.5)))
    factor = jnp.exp(jax.random.uniform(rough_key, (PAIRS, FREQ), jnp.float32, math.log(0.7), math.log(1.4)))
    return (scales * rising * factor).astype(jnp.float32)


def draw_taper_bank(key, part):
    floor_key = jax.random.fold_in(key, 31)
    power_key = jax.random.fold_in(key, 37)
    rough_key = jax.random.fold_in(key, 41)
    channel = (jnp.arange(FREQ, dtype=jnp.float32) + 0.5) / FREQ
    floors = jax.random.uniform(floor_key, (TAPERS, 1), jnp.float32, 0.25, 0.5)
    powers = jax.random.uniform(power_key, (TAPERS, 1), jnp.float32, 1.0, 2.0)
    hann_shape = jnp.sin(jnp.pi * channel)[None, :] ** 2
    smooth = floors + (1.0 - floors) * hann_shape ** powers
    rough_part = jnp.exp(jax.random.uniform(rough_key, (TAPERS, FREQ), jnp.float32, math.log(0.8), math.log(1.0)))
    return (smooth * rough_part * 1.25).astype(jnp.float32)


def touch_ends(drawn, stream_key, low, top_value):
    longest = drawn.shape.index(max(drawn.shape))
    spots = []
    for shift in (0, 1):
        where = [jax.random.randint(jax.random.fold_in(stream_key, axis), (), 0, length) for axis, length in enumerate(drawn.shape)]
        where[longest] = (where[longest] + shift) % drawn.shape[longest]
        spots.append(tuple(where))
    return drawn.at[spots[0]].set(low).at[spots[1]].set(top_value)


def steps_of(rng, extent, split, least, largest):
    def one(dim, shards_of):
        draws = jax.random.uniform(jax.random.fold_in(jax.random.fold_in(rng, 6), dim), (shards_of,), jnp.float32, least / len(split), largest / len(split))
        return jnp.repeat(jnp.exp(draws), extent[dim] // shards_of).reshape((-1,) + (1,) * (len(extent) - dim - 1))

    gain = one(*split[0])
    for cut in split[1:]:
        gain = gain * one(*cut)
    return gain


def bell_draw(own_key, extent, width, most, split=(), held_as=jnp.bfloat16):
    array = width * jax.random.normal(own_key, extent, jnp.float32)
    if split:
        array = array * steps_of(own_key, extent, split, -0.22, 0.18)
    return jnp.clip(array, -most, most).astype(held_as)


def setup_inputs(seed: int = 0) -> dict:
    key_list = jax.random.split(jax.random.key(seed), 6)
    vis = bell_draw(key_list[0], (PAIRS, 2, FREQ), 1.0, 6.0, ((0, 32),))
    inv_noise = draw_inv_noise(jax.random.fold_in(key_list[5], 71), 0)
    assign = draw_assign(jax.random.fold_in(key_list[5], 71), 0)
    taper_bank = draw_taper_bank(jax.random.fold_in(key_list[5], 71), 0)
    taper_pick = touch_ends(jax.random.randint(key_list[4], (WINDOWS,), 0, TAPERS), jax.random.fold_in(key_list[4], 1), 0, TAPERS - 1).astype(jnp.int32)
    return dict(vis=vis, inv_noise=inv_noise, assign=assign, taper_bank=taper_bank, taper_pick=taper_pick)


ridge_share = 0.1

def delay_table():
    delays = jnp.arange(P_SIZE, dtype=jnp.int32)
    channel = jnp.arange(FREQ, dtype=jnp.int32)
    phases = (delays[:, None] * channel[None, :] % FREQ).astype(jnp.float32) * (2.0 * jnp.pi / FREQ)
    cosine_rows = jnp.cos(phases).astype(jnp.bfloat16).T
    sine_rows = jnp.sin(phases).astype(jnp.bfloat16).T
    top_block = jnp.concatenate([cosine_rows, -sine_rows], axis=1)
    low_block = jnp.concatenate([sine_rows, cosine_rows], axis=1)
    return jnp.concatenate([top_block, low_block], axis=0)

def reference(vis, inv_noise, assign, taper_bank, taper_pick):
    delay_matrix = delay_table().astype(jnp.float32)
    devices = PAIRS // PAIR_DEV

    def transform(block_parts):
        vis_block, noise_block, pair_ids = block_parts
        taper_rows = taper_bank[taper_pick[pair_ids // 2]]
        weighted = (taper_rows[:, None, :] * noise_block[:, None, :] * vis_block.astype(jnp.float32)).astype(jnp.bfloat16)
        flat = weighted.reshape(PAIR_DEV, 2 * FREQ).astype(jnp.float32)
        return jnp.dot(flat.astype(jnp.float32), delay_matrix.astype(jnp.float32), precision=lax.Precision.HIGHEST, preferred_element_type=jnp.float32).astype(jnp.bfloat16)
    spectra = lax.map(transform, (vis.reshape(devices, PAIR_DEV, 2, FREQ), inv_noise.reshape(devices, PAIR_DEV, FREQ), assign.reshape(devices, PAIR_DEV)))
    spectra = spectra.reshape(PAIRS, 2 * P_SIZE)
    sort_order = jnp.argsort(assign, stable=True).astype(jnp.int32)
    ordered = jnp.concatenate([spectra[sort_order], jnp.zeros((PAIR_DEV, 2 * P_SIZE), spectra.dtype)], axis=0)
    counts = jax.ops.segment_sum(jnp.ones((PAIRS,), jnp.int32), assign, num_segments=2 * WINDOWS).astype(jnp.int32)
    starts = (jnp.cumsum(counts) - counts).astype(jnp.int32)

    def group_power(window, group):
        group_ident = (2 * window + group).astype(jnp.int32)
        group_rows = lax.dynamic_slice_in_dim(ordered, starts[group_ident], PAIR_DEV, 0)
        live_rows = (jnp.arange(PAIR_DEV, dtype=jnp.int32) < counts[group_ident])[:, None]
        group_rows = jnp.where(live_rows, group_rows, jnp.zeros_like(group_rows)).astype(jnp.float32)
        moments = lax.dot_general(group_rows.astype(jnp.float32), group_rows.astype(jnp.float32), (((0,), (0,)), ((), ())), precision=lax.Precision.HIGHEST, preferred_element_type=jnp.float32)
        real_part = moments[:P_SIZE, :P_SIZE] + moments[P_SIZE:, P_SIZE:]
        imag_part = moments[P_SIZE:, :P_SIZE] - moments[:P_SIZE, P_SIZE:]
        return (real_part, imag_part)

    def one_window(window):
        first_real, first_imag = group_power(window, 0)
        second_real, second_imag = group_power(window, 1)
        return 0.5 * (first_real * second_real + first_imag * second_imag)
    fisher = lax.map(one_window, jnp.arange(WINDOWS, dtype=jnp.int32))
    diag_total = jnp.sum(jnp.trace(fisher, axis1=1, axis2=2))
    ridge_term = ridge_share * diag_total / (WINDOWS * P_SIZE)

    def normalize(matrix):
        factor = jnp.linalg.cholesky(matrix + ridge_term * jnp.eye(P_SIZE, dtype=jnp.float32))
        window = factor.T
        row_sums = jnp.sum(window, axis=1)
        divisor = jnp.maximum(row_sums, jnp.diagonal(window))
        return window / divisor[:, None]
    return lax.map(normalize, fisher)
```

```python
import jax
import jax.numpy as jnp
from jax import lax
from jax.experimental import pallas as pl
from jax.experimental.pallas import tpu as pltpu
from jax.sharding import PartitionSpec as P

FREQ = 1024
P_SIZE = 512
TAPERS = 4


ridge_share = 0.1


def delay_table():
    delays = jnp.arange(P_SIZE, dtype=jnp.int32)
    channel = jnp.arange(FREQ, dtype=jnp.int32)
    phases = (delays[:, None] * channel[None, :] % FREQ).astype(jnp.float32) * (2.0 * jnp.pi / FREQ)
    cosine_rows = jnp.cos(phases).astype(jnp.bfloat16).T
    sine_rows = jnp.sin(phases).astype(jnp.bfloat16).T
    top_block = jnp.concatenate([cosine_rows, -sine_rows], axis=1)
    low_block = jnp.concatenate([sine_rows, cosine_rows], axis=1)
    return jnp.concatenate([top_block, low_block], axis=0)


STEP = 16
LANE = 128


def split_halves(x):
    high = x.astype(jnp.bfloat16)
    low = (x - high.astype(jnp.float32)).astype(jnp.bfloat16)
    return high, low


def cross(left, right):
    return lax.dot_general(left, right, (((0,), (0,)), ((), ())), preferred_element_type=jnp.float32)


def factor_kernel(ridge_ref, fisher_ref, out_ref, work_ref, left_ref, right_ref):
    size = fisher_ref.shape[0]
    ridge = ridge_ref[0:1, 0:1]
    rows = lax.broadcasted_iota(jnp.int32, (STEP, LANE), 0)
    lanes = lax.broadcasted_iota(jnp.int32, (STEP, LANE), 1)
    square_r = lax.broadcasted_iota(jnp.int32, (LANE, LANE), 0)
    square_c = lax.broadcasted_iota(jnp.int32, (LANE, LANE), 1)
    eye = jnp.where(square_r == square_c, jnp.broadcast_to(ridge, (LANE, LANE)), 0.0)
    for p in range(size // LANE):
        base = p * LANE
        tail = slice(base, base + LANE)
        work_ref[tail, base:] = fisher_ref[tail, base:]
        work_ref[tail, tail] = fisher_ref[tail, tail] + eye
    for p in range(size // LANE):
        base = p * LANE
        tiles = (size - base) // LANE
        for b in range(LANE // STEP):
            k = base + STEP * b
            panel = [work_ref[k : k + STEP, base + LANE * t : base + LANE * (t + 1)] for t in range(tiles)]
            columns = [
                jnp.broadcast_to(panel[0][:, STEP * b + c : STEP * b + c + 1], (STEP, LANE)) for c in range(STEP)
            ]
            scale = jnp.zeros((STEP, LANE), jnp.float32)
            for j in range(STEP):
                pivot = jnp.broadcast_to(columns[j][j : j + 1, :], (STEP, LANE))
                root = lax.rsqrt(pivot)
                scale = jnp.where(rows == j, root, scale)
                if j < STEP - 1:
                    ratio = jnp.where(rows > j, columns[j] * (root * root), 0.0)
                    for c in range(j + 1, STEP):
                        columns[c] = columns[c] - ratio * jnp.broadcast_to(columns[c][j : j + 1, :], (STEP, LANE))
                    panel = [x - ratio * jnp.broadcast_to(x[j : j + 1, :], (STEP, LANE)) for x in panel]
            panel = [x * scale for x in panel]
            panel[0] = jnp.where(lanes >= rows + STEP * b, panel[0], 0.0)
            halves = [split_halves(x) for x in panel]
            span = slice(STEP * b, STEP * (b + 1))
            if b < LANE // STEP - 1:
                left = jnp.concatenate([halves[0][0], halves[0][0], halves[0][1]], axis=0)
                for t in range(tiles):
                    right = jnp.concatenate([halves[t][0], halves[t][1], halves[t][0]], axis=0)
                    update = cross(left, right)
                    below = slice(k + STEP, base + LANE)
                    across = slice(base + LANE * t, base + LANE * (t + 1))
                    work_ref[below, across] = work_ref[below, across] - update[STEP * (b + 1) :, :]
            for t in range(1, tiles):
                across = slice(base + LANE * t, base + LANE * (t + 1))
                left_ref[span, across] = halves[t][0]
                right_ref[span, across] = halves[t][1]
            total = panel[0]
            for x in panel[1:]:
                total = total + x
            sums = jnp.sum(total, axis=1, keepdims=True)
            peak = jnp.sum(jnp.where(lanes == rows + STEP * b, panel[0], 0.0), axis=1, keepdims=True)
            inverse = jnp.broadcast_to(1.0 / jnp.maximum(sums, peak), (STEP, LANE))
            for t in range(p):
                out_ref[k : k + STEP, LANE * t : LANE * (t + 1)] = jnp.zeros((STEP, LANE), jnp.float32)
            for t in range(tiles):
                out_ref[k : k + STEP, base + LANE * t : base + LANE * (t + 1)] = panel[t] * inverse
        for q in range(p + 1, size // LANE):
            mine = slice(LANE * q, LANE * (q + 1))
            rest = slice(LANE * q, size)
            high, low = left_ref[:, mine], right_ref[:, mine]
            left = jnp.concatenate([high, high, low], axis=0)
            right = jnp.concatenate([left_ref[:, rest], right_ref[:, rest], left_ref[:, rest]], axis=0)
            work_ref[mine, rest] = work_ref[mine, rest] - cross(left, right)


def factor_rows(fisher, ridge):
    size = fisher.shape[0]
    return pl.pallas_call(
        factor_kernel,
        out_shape=jax.ShapeDtypeStruct((size, size), jnp.float32),
        in_specs=[pl.BlockSpec(memory_space=pltpu.VMEM)] * 2,
        out_specs=pl.BlockSpec(memory_space=pltpu.VMEM),
        scratch_shapes=[
            pltpu.VMEM((size, size), jnp.float32),
            pltpu.VMEM((LANE, size), jnp.bfloat16),
            pltpu.VMEM((LANE, size), jnp.bfloat16),
        ],
        name="factor_rows",
    )(jnp.broadcast_to(ridge, (8, LANE)), fisher)


def local(vis, inv_noise, assign, taper_bank, taper_pick):
    win_size = lax.axis_size("win")
    band_size = lax.axis_size("band")
    windows = win_size * band_size
    pair_count = assign.shape[0]
    capacity = pair_count // windows
    spectral = 2 * P_SIZE
    group_lanes = 2 * windows
    window_ids = assign // 2
    window_match = (window_ids[:, None] == jnp.arange(windows, dtype=jnp.int32)[None, :]).astype(
        jnp.int32
    )
    picked_taper = jnp.sum(window_match * taper_pick[None, :], axis=1)
    taper_match = (picked_taper[:, None] == jnp.arange(TAPERS, dtype=jnp.int32)[None, :]).astype(
        jnp.float32
    )
    taper_rows = jnp.dot(
        taper_match, taper_bank, precision=lax.Precision.HIGHEST, preferred_element_type=jnp.float32
    )
    weighted = (taper_rows[:, None, :] * inv_noise[:, None, :] * vis.astype(jnp.float32)).astype(
        jnp.bfloat16
    )
    spectra = jnp.dot(
        weighted.reshape(pair_count, 2 * FREQ), delay_table(), preferred_element_type=jnp.float32
    ).astype(jnp.bfloat16)
    ident_match = (assign[:, None] == jnp.arange(group_lanes, dtype=jnp.int32)[None, :]).astype(
        jnp.bfloat16
    )
    position = jnp.arange(pair_count, dtype=jnp.int32)
    before = (position[None, :] < position[:, None]).astype(jnp.bfloat16)
    earlier = jnp.dot(before, ident_match, preferred_element_type=jnp.float32)
    slot_rank = jnp.sum(earlier * ident_match.astype(jnp.float32), axis=1).astype(jnp.int32)
    slot_index = assign * capacity + slot_rank
    source_row = (
        jnp.full((group_lanes * capacity,), pair_count, jnp.int32).at[slot_index].set(position)
    )
    padded = jnp.concatenate([spectra, jnp.zeros((1, spectral), jnp.bfloat16)], axis=0)
    outgoing = jnp.take(padded, source_row, axis=0)
    incoming = lax.all_to_all(outgoing, ("win", "band"), split_axis=0, concat_axis=0, tiled=True)
    incoming = incoming.reshape(windows, 2, capacity, spectral)
    moments = jnp.einsum("sgcm,sgcn->gmn", incoming, incoming, preferred_element_type=jnp.float32)
    real_part = moments[:, :P_SIZE, :P_SIZE] + moments[:, P_SIZE:, P_SIZE:]
    imag_part = moments[:, P_SIZE:, :P_SIZE] - moments[:, :P_SIZE, P_SIZE:]
    fisher = 0.5 * (real_part[0] * real_part[1] + imag_part[0] * imag_part[1])
    local_trace = jnp.trace(fisher)
    shared = jnp.broadcast_to(local_trace, (windows,))
    diag_total = jnp.sum(lax.all_to_all(shared, ("win", "band"), 0, 0, tiled=True))
    ridge_term = ridge_share * diag_total / (windows * P_SIZE)
    return factor_rows(fisher, ridge_term)[None]


def solution(mesh):
    in_specs = (
        P(("win", "band"), None, None),
        P(("win", "band"), None),
        P(("win", "band")),
        P(),
        P(),
    )
    out_specs = P(("win", "band"), None, None)
    return jax.shard_map(local, mesh=mesh, in_specs=in_specs, out_specs=out_specs, check_vma=False)
```

```python
import functools

import jax
import jax.numpy as jnp
import numpy as np
from jax import lax
from jax.experimental import pallas as pl
from jax.experimental.pallas import tpu as pltpu
from jax.sharding import PartitionSpec as P

FREQ = 1024
P_SIZE = 512
TAPERS = 4


ridge_share = 0.1


STEP = 16
LANE = 128


def split_halves(x):
    high = x.astype(jnp.bfloat16)
    low = (x - high.astype(jnp.float32)).astype(jnp.bfloat16)
    return high, low


def cross(left, right):
    return lax.dot_general(left, right, (((0,), (0,)), ((), ())), preferred_element_type=jnp.float32)


def factor_kernel(trace_ref, fisher_ref, out_ref, work_ref, left_ref, right_ref):
    size = fisher_ref.shape[0]
    windows = trace_ref.shape[0]
    lane_total = jnp.sum(trace_ref[...], axis=0)
    ridge = jnp.sum(lane_total, axis=1, keepdims=True) * (ridge_share / (windows * size))
    rows = lax.broadcasted_iota(jnp.int32, (STEP, LANE), 0)
    lanes = lax.broadcasted_iota(jnp.int32, (STEP, LANE), 1)
    square_r = lax.broadcasted_iota(jnp.int32, (LANE, LANE), 0)
    square_c = lax.broadcasted_iota(jnp.int32, (LANE, LANE), 1)
    eye = jnp.where(square_r == square_c, jnp.broadcast_to(ridge, (LANE, LANE)), 0.0)
    for p in range(size // LANE):
        base = p * LANE
        tail = slice(base, base + LANE)
        work_ref[tail, base:] = fisher_ref[tail, base:]
        work_ref[tail, tail] = fisher_ref[tail, tail] + eye
    for p in range(size // LANE):
        base = p * LANE
        tiles = (size - base) // LANE
        for b in range(LANE // STEP):
            k = base + STEP * b
            panel = [work_ref[k : k + STEP, base + LANE * t : base + LANE * (t + 1)] for t in range(tiles)]
            columns = [
                jnp.broadcast_to(panel[0][:, STEP * b + c : STEP * b + c + 1], (STEP, LANE)) for c in range(STEP)
            ]
            scale = jnp.zeros((STEP, LANE), jnp.float32)
            for j in range(STEP):
                pivot = jnp.broadcast_to(columns[j][j : j + 1, :], (STEP, LANE))
                root = lax.rsqrt(pivot)
                scale = jnp.where(rows == j, root, scale)
                if j < STEP - 1:
                    ratio = jnp.where(rows > j, columns[j] * (root * root), 0.0)
                    for c in range(j + 1, STEP):
                        columns[c] = columns[c] - ratio * jnp.broadcast_to(columns[c][j : j + 1, :], (STEP, LANE))
                    panel = [x - ratio * jnp.broadcast_to(x[j : j + 1, :], (STEP, LANE)) for x in panel]
            panel = [x * scale for x in panel]
            panel[0] = jnp.where(lanes >= rows + STEP * b, panel[0], 0.0)
            halves = [split_halves(x) for x in panel]
            span = slice(STEP * b, STEP * (b + 1))
            if b < LANE // STEP - 1:
                left = jnp.concatenate([halves[0][0], halves[0][0], halves[0][1]], axis=0)
                for t in range(tiles):
                    right = jnp.concatenate([halves[t][0], halves[t][1], halves[t][0]], axis=0)
                    update = cross(left, right)
                    below = slice(k + STEP, base + LANE)
                    across = slice(base + LANE * t, base + LANE * (t + 1))
                    work_ref[below, across] = work_ref[below, across] - update[STEP * (b + 1) :, :]
            for t in range(1, tiles):
                across = slice(base + LANE * t, base + LANE * (t + 1))
                left_ref[span, across] = halves[t][0]
                right_ref[span, across] = halves[t][1]
            total = panel[0]
            for x in panel[1:]:
                total = total + x
            sums = jnp.sum(total, axis=1, keepdims=True)
            peak = jnp.sum(jnp.where(lanes == rows + STEP * b, panel[0], 0.0), axis=1, keepdims=True)
            inverse = jnp.broadcast_to(1.0 / jnp.maximum(sums, peak), (STEP, LANE))
            for t in range(p):
                out_ref[k : k + STEP, LANE * t : LANE * (t + 1)] = jnp.zeros((STEP, LANE), jnp.float32)
            for t in range(tiles):
                out_ref[k : k + STEP, base + LANE * t : base + LANE * (t + 1)] = panel[t] * inverse
        for q in range(p + 1, size // LANE):
            mine = slice(LANE * q, LANE * (q + 1))
            rest = slice(LANE * q, size)
            high, low = left_ref[:, mine], right_ref[:, mine]
            left = jnp.concatenate([high, high, low], axis=0)
            right = jnp.concatenate([left_ref[:, rest], right_ref[:, rest], left_ref[:, rest]], axis=0)
            work_ref[mine, rest] = work_ref[mine, rest] - cross(left, right)


def factor_rows(fisher, traces):
    size = fisher.shape[0]
    return pl.pallas_call(
        factor_kernel,
        out_shape=jax.ShapeDtypeStruct((size, size), jnp.float32),
        in_specs=[pl.BlockSpec(memory_space=pltpu.VMEM)] * 2,
        out_specs=pl.BlockSpec(memory_space=pltpu.VMEM),
        scratch_shapes=[
            pltpu.VMEM((size, size), jnp.float32),
            pltpu.VMEM((LANE, size), jnp.bfloat16),
            pltpu.VMEM((LANE, size), jnp.bfloat16),
        ],
        name="factor_rows",
    )(traces, fisher)


ROWS = 256
SLOTS = 256


def delay_parts():
    delays = np.arange(P_SIZE, dtype=np.int64)
    channel = np.arange(FREQ, dtype=np.int64)
    phases = (channel[:, None] * delays[None, :] % FREQ).astype(np.float32) * np.float32(2.0 * np.pi / FREQ)
    both = np.concatenate([np.cos(phases), np.sin(phases)], axis=0)
    return jnp.asarray(both.astype(np.float32)).astype(jnp.bfloat16)


def front_kernel(steps, capacity, vis_ref, noise_ref, column_ref, row_ref, pick_ref, bank_ref, table_ref, out_ref, spectra_ref, slot_ref):
    step = pl.program_id(0)
    windows = pick_ref.shape[1]

    @pl.when(step < steps)
    def transform():
        ids = column_ref[...]
        lanes = lax.broadcasted_iota(jnp.int32, (ROWS, windows), 1)
        hit = jnp.broadcast_to(ids // 2, (ROWS, windows)) == lanes
        picks = jnp.broadcast_to(pick_ref[...], (ROWS, windows))
        pick = jnp.sum(jnp.where(hit, picks, 0), axis=1, keepdims=True)
        taper = jnp.broadcast_to(bank_ref[0:1, :], (ROWS, FREQ))
        for t in range(1, TAPERS):
            taper = jnp.where(pick == t, bank_ref[t : t + 1, :], taper)
        weight = taper * noise_ref[...]
        real = (weight * vis_ref[:, 0, :].astype(jnp.float32)).astype(jnp.bfloat16)
        imag = (weight * vis_ref[:, 1, :].astype(jnp.float32)).astype(jnp.bfloat16)
        left = jnp.concatenate(
            [jnp.concatenate([real, imag], axis=1), jnp.concatenate([imag, -real], axis=1)], axis=0
        )
        both = jnp.dot(left, table_ref[...], preferred_element_type=jnp.float32).astype(jnp.bfloat16)
        here = pl.ds(pl.multiple_of(step * ROWS, ROWS), ROWS)
        spectra_ref[here, :P_SIZE] = both[:ROWS]
        spectra_ref[here, P_SIZE:] = both[ROWS:]

    @pl.when(step == 0)
    def rank():
        count = row_ref.shape[1]
        groups = 2 * windows
        ids = row_ref[...]
        match = jnp.broadcast_to(ids, (groups, count)) == lax.broadcasted_iota(jnp.int32, (groups, count), 0)
        first = lax.broadcasted_iota(jnp.int32, (count, count), 0)
        second = lax.broadcasted_iota(jnp.int32, (count, count), 1)
        before = jnp.where(first < second, 1.0, 0.0).astype(jnp.bfloat16)
        member = jnp.where(match, 1.0, 0.0)
        earlier = jnp.dot(member.astype(jnp.bfloat16), before, preferred_element_type=jnp.float32)
        order = jnp.sum(member * earlier, axis=0, keepdims=True).astype(jnp.int32)
        slot_ref[...] = ids * capacity + order

    @pl.when(step >= steps)
    def place():
        count = row_ref.shape[1]
        first = (step - steps) * SLOTS
        wanted = lax.broadcasted_iota(jnp.int32, (SLOTS, count), 0) + first
        choose = jnp.where(jnp.broadcast_to(slot_ref[...], (SLOTS, count)) == wanted, 1.0, 0.0).astype(jnp.bfloat16)
        out_ref[...] = jnp.dot(choose, spectra_ref[...], preferred_element_type=jnp.float32).astype(jnp.bfloat16)


def outgoing_slots(vis, inv_noise, assign, taper_bank, taper_pick, windows, capacity):
    pair_count = assign.shape[0]
    steps = pair_count // ROWS
    slots = 2 * windows * capacity
    last = steps - 1

    def early(step):
        return jnp.minimum(step, last)

    return pl.pallas_call(
        functools.partial(front_kernel, steps, capacity),
        grid=(steps + slots // SLOTS,),
        out_shape=jax.ShapeDtypeStruct((slots, 2 * P_SIZE), jnp.bfloat16),
        in_specs=[
            pl.BlockSpec((ROWS, 2, FREQ), lambda s: (early(s), 0, 0)),
            pl.BlockSpec((ROWS, FREQ), lambda s: (early(s), 0)),
            pl.BlockSpec((ROWS, 1), lambda s: (early(s), 0)),
            pl.BlockSpec((1, pair_count), lambda s: (0, 0)),
            pl.BlockSpec((1, windows), lambda s: (0, 0)),
            pl.BlockSpec((TAPERS, FREQ), lambda s: (0, 0)),
            pl.BlockSpec((2 * FREQ, P_SIZE), lambda s: (0, 0)),
        ],
        out_specs=pl.BlockSpec((SLOTS, 2 * P_SIZE), lambda s: (jnp.maximum(s - steps, 0), 0)),
        scratch_shapes=[
            pltpu.VMEM((pair_count, 2 * P_SIZE), jnp.bfloat16),
            pltpu.VMEM((1, pair_count), jnp.int32),
        ],
        compiler_params=pltpu.CompilerParams(dimension_semantics=("arbitrary",)),
        name="front",
    )(vis, inv_noise, assign[:, None], assign[None, :], taper_pick[None, :], taper_bank, delay_parts())


def moment_kernel(rows_ref, fisher_ref, trace_ref, real_ref, imag_ref):
    sources, capacity, spectral = rows_ref.shape
    size = spectral // 2
    rows = rows_ref[...].reshape(sources * capacity, spectral)
    first, second = rows[:, :size], rows[:, size:]
    mixed = cross(second, rows)
    real = cross(first, first) + mixed[:, size:]
    imag = mixed[:, :size] - mixed[:, :size].T

    @pl.when(pl.program_id(0) == 0)
    def keep():
        real_ref[...] = real
        imag_ref[...] = imag

    @pl.when(pl.program_id(0) == 1)
    def combine():
        fisher = 0.5 * (real_ref[...] * real + imag_ref[...] * imag)
        fisher_ref[...] = fisher
        square_r = lax.broadcasted_iota(jnp.int32, (LANE, LANE), 0)
        square_c = lax.broadcasted_iota(jnp.int32, (LANE, LANE), 1)
        diagonal = jnp.zeros((LANE, LANE), jnp.float32)
        for p in range(size // LANE):
            span = slice(LANE * p, LANE * (p + 1))
            diagonal = diagonal + jnp.where(square_r == square_c, fisher[span, span], 0.0)
        lanes = jnp.sum(diagonal, axis=0, keepdims=True)
        trace_ref[...] = jnp.broadcast_to(lanes, trace_ref.shape)


def window_moments(incoming, windows):
    sources, both, spectral = incoming.shape
    size = spectral // 2
    capacity = both // 2
    return pl.pallas_call(
        moment_kernel,
        grid=(2,),
        out_shape=[
            jax.ShapeDtypeStruct((size, size), jnp.float32),
            jax.ShapeDtypeStruct((windows, 1, LANE), jnp.float32),
        ],
        in_specs=[pl.BlockSpec((sources, capacity, spectral), lambda g: (0, g, 0))],
        out_specs=[
            pl.BlockSpec((size, size), lambda g: (0, 0)),
            pl.BlockSpec((windows, 1, LANE), lambda g: (0, 0, 0)),
        ],
        scratch_shapes=[pltpu.VMEM((size, size), jnp.float32)] * 2,
        compiler_params=pltpu.CompilerParams(dimension_semantics=("arbitrary",)),
        name="moments",
    )(incoming)


def local(vis, inv_noise, assign, taper_bank, taper_pick):
    win_size = lax.axis_size("win")
    band_size = lax.axis_size("band")
    windows = win_size * band_size
    capacity = assign.shape[0] // windows
    spectral = 2 * P_SIZE
    outgoing = outgoing_slots(vis, inv_noise, assign, taper_bank, taper_pick, windows, capacity)
    incoming = lax.all_to_all(outgoing, ("win", "band"), split_axis=0, concat_axis=0, tiled=True)
    fisher, traces = window_moments(incoming.reshape(windows, 2 * capacity, spectral), windows)
    traces = lax.all_to_all(traces, ("win", "band"), split_axis=0, concat_axis=0, tiled=True)
    return factor_rows(fisher, traces)[None]


def solution(mesh):
    in_specs = (
        P(("win", "band"), None, None),
        P(("win", "band"), None),
        P(("win", "band")),
        P(),
        P(),
    )
    out_specs = P(("win", "band"), None, None)
    return jax.shard_map(local, mesh=mesh, in_specs=in_specs, out_specs=out_specs, check_vma=False)
```

```python
import functools

import jax
import jax.numpy as jnp
import numpy as np
from jax import lax
from jax.experimental import pallas as pl
from jax.experimental.pallas import tpu as pltpu
from jax.sharding import PartitionSpec as P

FREQ = 1024
P_SIZE = 512
TAPERS = 4


ridge_share = 0.1


STEP = 16
LANE = 128


def split_halves(x):
    high = x.astype(jnp.bfloat16)
    low = (x - high.astype(jnp.float32)).astype(jnp.bfloat16)
    return high, low


def cross(left, right):
    return lax.dot_general(left, right, (((0,), (0,)), ((), ())), preferred_element_type=jnp.float32)


def factor_kernel(trace_ref, near_ref, far_first_ref, far_second_ref, out_ref, work_ref, left_ref, right_ref):
    size = out_ref.shape[0]
    windows = trace_ref.shape[0]
    lane_total = jnp.sum(trace_ref[...], axis=0)
    ridge = jnp.sum(lane_total, axis=1, keepdims=True) * (ridge_share / (windows * size))
    rows = lax.broadcasted_iota(jnp.int32, (STEP, LANE), 0)
    lanes = lax.broadcasted_iota(jnp.int32, (STEP, LANE), 1)
    square_r = lax.broadcasted_iota(jnp.int32, (LANE, LANE), 0)
    square_c = lax.broadcasted_iota(jnp.int32, (LANE, LANE), 1)
    ridges = jnp.broadcast_to(ridge, (LANE, LANE))

    def product(p, q):
        mine, across = slice(LANE * p, LANE * (p + 1)), slice(LANE * q, LANE * (q + 1))
        first = near_ref[0, mine, across] + far_first_ref[0, mine, across].astype(jnp.float32)
        second = near_ref[1, mine, across] + far_second_ref[0, mine, across].astype(jnp.float32)
        return 0.5 * first * second

    for p in range(size // LANE):
        mine = slice(LANE * p, LANE * (p + 1))
        block = product(p, p)
        work_ref[mine, mine] = jnp.where(square_r == square_c, block + ridges, block + block.T)
        for q in range(p + 1, size // LANE):
            work_ref[mine, LANE * q : LANE * (q + 1)] = product(p, q) + product(q, p).T
    for p in range(size // LANE):
        base = p * LANE
        tiles = (size - base) // LANE
        for b in range(LANE // STEP):
            k = base + STEP * b
            panel = [work_ref[k : k + STEP, base + LANE * t : base + LANE * (t + 1)] for t in range(tiles)]
            columns = [
                jnp.broadcast_to(panel[0][:, STEP * b + c : STEP * b + c + 1], (STEP, LANE)) for c in range(STEP)
            ]
            scale = jnp.zeros((STEP, LANE), jnp.float32)
            for j in range(STEP):
                pivot = jnp.broadcast_to(columns[j][j : j + 1, :], (STEP, LANE))
                root = lax.rsqrt(pivot)
                scale = jnp.where(rows == j, root, scale)
                if j < STEP - 1:
                    ratio = jnp.where(rows > j, columns[j] * (root * root), 0.0)
                    for c in range(j + 1, STEP):
                        columns[c] = columns[c] - ratio * jnp.broadcast_to(columns[c][j : j + 1, :], (STEP, LANE))
                    panel = [x - ratio * jnp.broadcast_to(x[j : j + 1, :], (STEP, LANE)) for x in panel]
            panel = [x * scale for x in panel]
            panel[0] = jnp.where(lanes >= rows + STEP * b, panel[0], 0.0)
            halves = [split_halves(x) for x in panel]
            span = slice(STEP * b, STEP * (b + 1))
            if b < LANE // STEP - 1:
                left = jnp.concatenate([halves[0][0], halves[0][0], halves[0][1]], axis=0)
                for t in range(tiles):
                    right = jnp.concatenate([halves[t][0], halves[t][1], halves[t][0]], axis=0)
                    update = cross(left, right)
                    below = slice(k + STEP, base + LANE)
                    across = slice(base + LANE * t, base + LANE * (t + 1))
                    work_ref[below, across] = work_ref[below, across] - update[STEP * (b + 1) :, :]
            for t in range(1, tiles):
                across = slice(base + LANE * t, base + LANE * (t + 1))
                left_ref[span, across] = halves[t][0]
                right_ref[span, across] = halves[t][1]
            total = panel[0]
            for x in panel[1:]:
                total = total + x
            sums = jnp.sum(total, axis=1, keepdims=True)
            peak = jnp.sum(jnp.where(lanes == rows + STEP * b, panel[0], 0.0), axis=1, keepdims=True)
            inverse = jnp.broadcast_to(1.0 / jnp.maximum(sums, peak), (STEP, LANE))
            for t in range(p):
                out_ref[k : k + STEP, LANE * t : LANE * (t + 1)] = jnp.zeros((STEP, LANE), jnp.float32)
            for t in range(tiles):
                out_ref[k : k + STEP, base + LANE * t : base + LANE * (t + 1)] = panel[t] * inverse
        for q in range(p + 1, size // LANE):
            mine = slice(LANE * q, LANE * (q + 1))
            rest = slice(LANE * q, size)
            high, low = left_ref[:, mine], right_ref[:, mine]
            left = jnp.concatenate([high, high, low], axis=0)
            right = jnp.concatenate([left_ref[:, rest], right_ref[:, rest], left_ref[:, rest]], axis=0)
            work_ref[mine, rest] = work_ref[mine, rest] - cross(left, right)


def factor_rows(traces, near, first, second):
    size = near.shape[1]
    return pl.pallas_call(
        factor_kernel,
        out_shape=jax.ShapeDtypeStruct((size, size), jnp.float32),
        in_specs=[pl.BlockSpec(memory_space=pltpu.VMEM)] * 4,
        out_specs=pl.BlockSpec(memory_space=pltpu.VMEM),
        scratch_shapes=[
            pltpu.VMEM((size, size), jnp.float32),
            pltpu.VMEM((LANE, size), jnp.bfloat16),
            pltpu.VMEM((LANE, size), jnp.bfloat16),
        ],
        name="factor_rows",
    )(traces, near, first, second)


ROWS = 256
SLOTS = 512


def delay_parts():
    delays = np.arange(P_SIZE, dtype=np.int64)
    channel = np.arange(FREQ // 2, dtype=np.int64)
    phases = (channel[:, None] * delays[None, :] % FREQ).astype(np.float32) * np.float32(2.0 * np.pi / FREQ)
    both = np.concatenate([np.cos(phases), np.sin(phases)], axis=0)
    return jnp.asarray(both.astype(np.float32)).astype(jnp.bfloat16)


def front_kernel(steps, capacity, quarter, vis_ref, noise_ref, part_ref, row_ref, pick_ref, bank_ref, parts_ref, first_ref, second_ref, spectra_ref, slot_ref, table_ref):
    step = pl.program_id(0)
    windows = pick_ref.shape[1]

    @pl.when(step == 0)
    def fill():
        near = FREQ // 2
        odd = lax.broadcasted_iota(jnp.int32, (near, P_SIZE), 1) & 1
        for t in range(2):
            part = parts_ref[near * t : near * (t + 1), :]
            table_ref[FREQ * t : FREQ * t + near, :] = part
            table_ref[FREQ * t + near : FREQ * (t + 1), :] = jnp.where(odd == 1, -part, part)

    @pl.when(step < steps)
    def transform():
        ids = jnp.broadcast_to(part_ref[...], (8, ROWS)).T[:, 0:1]
        lanes = lax.broadcasted_iota(jnp.int32, (ROWS, windows), 1)
        hit = jnp.broadcast_to(ids // 2, (ROWS, windows)) == lanes
        picks = jnp.broadcast_to(pick_ref[...], (ROWS, windows))
        pick = jnp.sum(jnp.where(hit, picks, 0), axis=1, keepdims=True)
        taper = jnp.broadcast_to(bank_ref[0:1, :], (ROWS, FREQ))
        for t in range(1, TAPERS):
            taper = jnp.where(pick == t, bank_ref[t : t + 1, :], taper)
        weight = taper * noise_ref[...]
        real = (weight * vis_ref[:, 0, :].astype(jnp.float32)).astype(jnp.bfloat16)
        imag = (weight * vis_ref[:, 1, :].astype(jnp.float32)).astype(jnp.bfloat16)
        left = jnp.concatenate(
            [jnp.concatenate([real, imag], axis=1), jnp.concatenate([imag, -real], axis=1)], axis=0
        )
        both = jnp.dot(left, table_ref[...], preferred_element_type=jnp.float32).astype(jnp.bfloat16)
        here = pl.ds(pl.multiple_of(step * ROWS, ROWS), ROWS)
        spectra_ref[here, :P_SIZE] = both[:ROWS]
        spectra_ref[here, P_SIZE:] = both[ROWS:]

    @pl.when(step == 0)
    def rank():
        count = row_ref.shape[1]
        groups = 2 * windows
        names = row_ref[...]
        match = jnp.broadcast_to(names, (groups, count)) == lax.broadcasted_iota(jnp.int32, (groups, count), 0)
        first = lax.broadcasted_iota(jnp.int32, (count, count), 0)
        second = lax.broadcasted_iota(jnp.int32, (count, count), 1)
        before = jnp.where(first < second, 1.0, 0.0).astype(jnp.bfloat16)
        member = jnp.where(match, 1.0, 0.0)
        earlier = jnp.dot(member.astype(jnp.bfloat16), before, preferred_element_type=jnp.float32)
        order = jnp.sum(member * earlier, axis=0, keepdims=True).astype(jnp.int32)
        upper = lax.axis_index("win") * 2 >= lax.axis_size("win")
        shifted = jnp.where(names >= windows, names - windows, names + windows)
        ordered = jnp.where(upper, names, shifted)
        split = ((ordered & 1) * (windows // 2) + ordered // 2) * capacity
        slot_ref[...] = jnp.where(ordered < windows, split, ordered * capacity) + order

    @pl.when((step >= steps) & (step < steps + quarter))
    def first():
        first_ref[...] = placed_rows((step - steps) * SLOTS, slot_ref, spectra_ref)

    @pl.when(step >= steps + quarter)
    def second():
        second_ref[...] = placed_rows((step - steps) * SLOTS, slot_ref, spectra_ref)


def placed_rows(first, slot_ref, spectra_ref):
    count = slot_ref.shape[1]
    wanted = lax.broadcasted_iota(jnp.int32, (SLOTS, count), 0) + first
    choose = jnp.where(jnp.broadcast_to(slot_ref[...], (SLOTS, count)) == wanted, 1.0, 0.0).astype(jnp.bfloat16)
    return jnp.dot(choose, spectra_ref[...], preferred_element_type=jnp.float32).astype(jnp.bfloat16)


def near_kernel(offset, slot_ref, spectra_ref, out_ref):
    out_ref[...] = placed_rows(offset + pl.program_id(0) * SLOTS, slot_ref, spectra_ref)


def near_slots(slots, spectra, offset):
    count, spectral = spectra.shape
    return pl.pallas_call(
        functools.partial(near_kernel, offset),
        grid=(offset // SLOTS,),
        out_shape=jax.ShapeDtypeStruct((offset, spectral), jnp.bfloat16),
        in_specs=[pl.BlockSpec((1, count), lambda s: (0, 0)), pl.BlockSpec((count, spectral), lambda s: (0, 0))],
        out_specs=pl.BlockSpec((SLOTS, spectral), lambda s: (s, 0)),
        name="near",
    )(slots, spectra)


def far_slots(vis, inv_noise, assign, taper_bank, taper_pick, windows, capacity):
    pair_count = assign.shape[0]
    steps = pair_count // ROWS
    slots = windows * capacity // 2
    quarter = slots // SLOTS
    last = steps - 1
    names = assign[None, :]

    def early(step):
        return jnp.minimum(step, last)

    return pl.pallas_call(
        functools.partial(front_kernel, steps, capacity, quarter),
        grid=(steps + 2 * quarter,),
        out_shape=[
            jax.ShapeDtypeStruct((slots, 2 * P_SIZE), jnp.bfloat16),
            jax.ShapeDtypeStruct((slots, 2 * P_SIZE), jnp.bfloat16),
            jax.ShapeDtypeStruct((pair_count, 2 * P_SIZE), jnp.bfloat16),
            jax.ShapeDtypeStruct((1, pair_count), jnp.int32),
        ],
        in_specs=[
            pl.BlockSpec((ROWS, 2, FREQ), lambda s: (early(s), 0, 0)),
            pl.BlockSpec((ROWS, FREQ), lambda s: (early(s), 0)),
            pl.BlockSpec((1, ROWS), lambda s: (0, early(s))),
            pl.BlockSpec((1, pair_count), lambda s: (0, 0)),
            pl.BlockSpec((1, windows), lambda s: (0, 0)),
            pl.BlockSpec((TAPERS, FREQ), lambda s: (0, 0)),
            pl.BlockSpec((FREQ, P_SIZE), lambda s: (0, 0)),
        ],
        out_specs=[
            pl.BlockSpec((SLOTS, 2 * P_SIZE), lambda s: (jnp.clip(s - steps, 0, quarter - 1), 0)),
            pl.BlockSpec((SLOTS, 2 * P_SIZE), lambda s: (jnp.maximum(s - steps - quarter, 0), 0)),
            pl.BlockSpec((pair_count, 2 * P_SIZE), lambda s: (0, 0)),
            pl.BlockSpec((1, pair_count), lambda s: (0, 0)),
        ],
        scratch_shapes=[pltpu.VMEM((2 * FREQ, P_SIZE), jnp.bfloat16)],
        compiler_params=pltpu.CompilerParams(dimension_semantics=("arbitrary",)),
        name="front",
    )(vis, inv_noise, names, names, taper_pick[None, :], taper_bank, delay_parts())


def packed_moments(rows):
    sources, capacity, spectral = rows.shape
    size = spectral // 2
    rows = rows.reshape(sources * capacity, spectral)
    first, second = rows[:, :size], rows[:, size:]
    mixed = cross(second, rows)
    real = cross(first, first) + mixed[:, size:]
    imag = mixed[:, :size] - mixed[:, :size].T
    r = lax.broadcasted_iota(jnp.int32, (size, size), 0)
    c = lax.broadcasted_iota(jnp.int32, (size, size), 1)
    packed = jnp.where(r <= c, real, imag)
    return packed, jnp.sum(jnp.where(r == c, real, 0.0), axis=0, keepdims=True)


def far_kernel(rows_ref, packed_ref, power_ref):
    packed, power = packed_moments(rows_ref[...])
    packed_ref[0] = packed.astype(jnp.bfloat16)
    power_ref[0] = power


def near_moment_kernel(rows_ref, first_ref, second_ref, packed_ref, trace_ref, power_ref):
    packed, power = packed_moments(rows_ref[...])
    packed_ref[0] = packed
    total = power + jnp.where(pl.program_id(0) == 0, first_ref[0], second_ref[0])

    @pl.when(pl.program_id(0) == 0)
    def keep():
        power_ref[...] = total

    @pl.when(pl.program_id(0) == 1)
    def combine():
        both = 0.5 * power_ref[...] * total
        lanes = both[:, :LANE]
        for t in range(1, both.shape[1] // LANE):
            lanes = lanes + both[:, LANE * t : LANE * (t + 1)]
        trace_ref[...] = jnp.broadcast_to(lanes, trace_ref.shape)


def far_moments(incoming):
    _, _, spectral = incoming.shape
    size = spectral // 2
    return pl.pallas_call(
        far_kernel,
        out_shape=[
            jax.ShapeDtypeStruct((1, size, size), jnp.bfloat16),
            jax.ShapeDtypeStruct((1, 1, size), jnp.float32),
        ],
        name="far_moments",
    )(incoming)


def near_moments(incoming, first, second, windows):
    sources, both, spectral = incoming.shape
    size = spectral // 2
    power = pl.BlockSpec((1, 1, size), lambda g: (0, 0, 0))
    return pl.pallas_call(
        near_moment_kernel,
        grid=(2,),
        out_shape=[
            jax.ShapeDtypeStruct((2, size, size), jnp.float32),
            jax.ShapeDtypeStruct((windows, 1, LANE), jnp.float32),
        ],
        in_specs=[pl.BlockSpec((sources, both // 2, spectral), lambda g: (0, g, 0)), power, power],
        out_specs=[
            pl.BlockSpec((1, size, size), lambda g: (g, 0, 0)),
            pl.BlockSpec((windows, 1, LANE), lambda g: (0, 0, 0)),
        ],
        scratch_shapes=[pltpu.VMEM((1, size), jnp.float32)],
        compiler_params=pltpu.CompilerParams(dimension_semantics=("arbitrary",)),
        name="near_moments",
    )(incoming, first, second)


def local(vis, inv_noise, assign, taper_bank, taper_pick):
    win_size = lax.axis_size("win")
    band_size = lax.axis_size("band")
    windows = win_size * band_size
    capacity = assign.shape[0] // windows
    spectral = 2 * P_SIZE
    half = windows // 2
    groups = [list(range(half)), list(range(half, windows))]
    mirror = [(i, (i + half) % windows) for i in range(windows)]
    everywhere = ("win", "band")

    def gather_half(rows):
        rows = rows.reshape(half, rows.shape[0] // half, spectral)
        return lax.all_to_all(
            rows, everywhere, split_axis=0, concat_axis=0, axis_index_groups=groups, tiled=True
        )

    *fars, spectra, slots = far_slots(vis, inv_noise, assign, taper_bank, taper_pick, windows, capacity)
    near = near_slots(slots, spectra, windows * capacity)
    received, powers = [], []
    for far in fars:
        far = gather_half(far)
        packed, power = far_moments(far)
        powers.append(lax.ppermute(power, everywhere, mirror))
        received.append(lax.ppermute(packed, everywhere, mirror))
    near = gather_half(near)
    near, traces = near_moments(near, *powers, windows)
    traces = lax.all_to_all(traces, everywhere, split_axis=0, concat_axis=0, tiled=True)
    return factor_rows(traces, near, *received)[None]


def solution(mesh):
    in_specs = (
        P(("win", "band"), None, None),
        P(("win", "band"), None),
        P(("win", "band")),
        P(),
        P(),
    )
    out_specs = P(("win", "band"), None, None)
    return jax.shard_map(local, mesh=mesh, in_specs=in_specs, out_specs=out_specs, check_vma=False)
```

```python
import functools

import jax
import jax.numpy as jnp
import numpy as np
from jax import lax
from jax.experimental import pallas as pl
from jax.experimental.pallas import tpu as pltpu
from jax.sharding import PartitionSpec as P

FREQ = 1024
P_SIZE = 512
TAPERS = 4


ridge_share = 0.1


STEP = 16
LANE = 128


def split_halves(x):
    high = x.astype(jnp.bfloat16)
    low = (x - high.astype(jnp.float32)).astype(jnp.bfloat16)
    return high, low


def cross(left, right):
    return lax.dot_general(left, right, (((0,), (0,)), ((), ())), preferred_element_type=jnp.float32)


def factor_kernel(trace_ref, near_ref, far_first_ref, far_second_ref, out_ref, work_ref, left_ref, right_ref):
    size = out_ref.shape[0]
    windows = trace_ref.shape[0]
    lane_total = jnp.sum(trace_ref[...], axis=0)
    ridge = jnp.sum(lane_total, axis=1, keepdims=True) * (ridge_share / (windows * size))
    rows = lax.broadcasted_iota(jnp.int32, (STEP, LANE), 0)
    lanes = lax.broadcasted_iota(jnp.int32, (STEP, LANE), 1)
    square_r = lax.broadcasted_iota(jnp.int32, (LANE, LANE), 0)
    square_c = lax.broadcasted_iota(jnp.int32, (LANE, LANE), 1)
    ridges = jnp.broadcast_to(ridge, (LANE, LANE))

    def product(p, q):
        mine, across = slice(LANE * p, LANE * (p + 1)), slice(LANE * q, LANE * (q + 1))
        first = near_ref[0, mine, across] + far_first_ref[0, mine, across].astype(jnp.float32)
        second = near_ref[1, mine, across] + far_second_ref[0, mine, across].astype(jnp.float32)
        return 0.5 * first * second

    for p in range(size // LANE):
        mine = slice(LANE * p, LANE * (p + 1))
        block = product(p, p)
        work_ref[mine, mine] = jnp.where(square_r == square_c, block + ridges, block + block.T)
        for q in range(p + 1, size // LANE):
            work_ref[mine, LANE * q : LANE * (q + 1)] = product(p, q) + product(q, p).T
    for p in range(size // LANE):
        base = p * LANE
        tiles = (size - base) // LANE
        for b in range(LANE // STEP):
            k = base + STEP * b
            panel = [work_ref[k : k + STEP, base + LANE * t : base + LANE * (t + 1)] for t in range(tiles)]
            columns = [
                jnp.broadcast_to(panel[0][:, STEP * b + c : STEP * b + c + 1], (STEP, LANE)) for c in range(STEP)
            ]
            scale = jnp.zeros((STEP, LANE), jnp.float32)
            for j in range(STEP):
                pivot = jnp.broadcast_to(columns[j][j : j + 1, :], (STEP, LANE))
                root = lax.rsqrt(pivot)
                scale = jnp.where(rows == j, root, scale)
                if j < STEP - 1:
                    ratio = jnp.where(rows > j, columns[j] * (root * root), 0.0)
                    for c in range(j + 1, STEP):
                        columns[c] = columns[c] - ratio * jnp.broadcast_to(columns[c][j : j + 1, :], (STEP, LANE))
                    panel = [x - ratio * jnp.broadcast_to(x[j : j + 1, :], (STEP, LANE)) for x in panel]
            panel = [x * scale for x in panel]
            panel[0] = jnp.where(lanes >= rows + STEP * b, panel[0], 0.0)
            halves = [split_halves(x) for x in panel]
            span = slice(STEP * b, STEP * (b + 1))
            if b < LANE // STEP - 1:
                left = jnp.concatenate([halves[0][0], halves[0][0], halves[0][1]], axis=0)
                for t in range(tiles):
                    right = jnp.concatenate([halves[t][0], halves[t][1], halves[t][0]], axis=0)
                    update = cross(left, right)
                    below = slice(k + STEP, base + LANE)
                    across = slice(base + LANE * t, base + LANE * (t + 1))
                    work_ref[below, across] = work_ref[below, across] - update[STEP * (b + 1) :, :]
            for t in range(1, tiles):
                across = slice(base + LANE * t, base + LANE * (t + 1))
                left_ref[span, across] = halves[t][0]
                right_ref[span, across] = halves[t][1]
            total = panel[0]
            for x in panel[1:]:
                total = total + x
            sums = jnp.sum(total, axis=1, keepdims=True)
            peak = jnp.sum(jnp.where(lanes == rows + STEP * b, panel[0], 0.0), axis=1, keepdims=True)
            inverse = jnp.broadcast_to(1.0 / jnp.maximum(sums, peak), (STEP, LANE))
            for t in range(p):
                out_ref[k : k + STEP, LANE * t : LANE * (t + 1)] = jnp.zeros((STEP, LANE), jnp.float32)
            for t in range(tiles):
                out_ref[k : k + STEP, base + LANE * t : base + LANE * (t + 1)] = panel[t] * inverse
        for q in range(p + 1, size // LANE):
            mine = slice(LANE * q, LANE * (q + 1))
            rest = slice(LANE * q, size)
            high, low = left_ref[:, mine], right_ref[:, mine]
            left = jnp.concatenate([high, high, low], axis=0)
            right = jnp.concatenate([left_ref[:, rest], right_ref[:, rest], left_ref[:, rest]], axis=0)
            work_ref[mine, rest] = work_ref[mine, rest] - cross(left, right)


def factor_rows(traces, near, first, second):
    size = near.shape[1]
    return pl.pallas_call(
        factor_kernel,
        out_shape=jax.ShapeDtypeStruct((size, size), jnp.float32),
        in_specs=[pl.BlockSpec(memory_space=pltpu.VMEM)] * 4,
        out_specs=pl.BlockSpec(memory_space=pltpu.VMEM),
        scratch_shapes=[
            pltpu.VMEM((size, size), jnp.float32),
            pltpu.VMEM((LANE, size), jnp.bfloat16),
            pltpu.VMEM((LANE, size), jnp.bfloat16),
        ],
        name="factor_rows",
    )(traces, near, first, second)


ROWS = 256
SLOTS = 512


def delay_parts():
    delays = np.arange(P_SIZE, dtype=np.int64)
    channel = np.arange(FREQ // 2, dtype=np.int64)
    phases = (channel[:, None] * delays[None, :] % FREQ).astype(np.float32) * np.float32(2.0 * np.pi / FREQ)
    both = np.concatenate([np.cos(phases), np.sin(phases)], axis=0)
    return jnp.asarray(both.astype(np.float32)).astype(jnp.bfloat16)


def paired(windows):
    half = windows // 2
    return half <= 16 and half & (half - 1) == 0


def front_kernel(steps, capacity, quarter, vis_ref, noise_ref, part_ref, row_ref, pick_ref, bank_ref, parts_ref, first_ref, second_ref, spectra_ref, slot_ref, table_ref):
    step = pl.program_id(0)
    windows = pick_ref.shape[1]

    @pl.when(step == 0)
    def fill():
        near = FREQ // 2
        odd = lax.broadcasted_iota(jnp.int32, (near, P_SIZE), 1) & 1
        for t in range(2):
            part = parts_ref[near * t : near * (t + 1), :]
            table_ref[FREQ * t : FREQ * t + near, :] = part
            table_ref[FREQ * t + near : FREQ * (t + 1), :] = jnp.where(odd == 1, -part, part)

    @pl.when(step < steps)
    def transform():
        ids = jnp.broadcast_to(part_ref[...], (8, ROWS)).T[:, 0:1]
        lanes = lax.broadcasted_iota(jnp.int32, (ROWS, windows), 1)
        hit = jnp.broadcast_to(ids // 2, (ROWS, windows)) == lanes
        picks = jnp.broadcast_to(pick_ref[...], (ROWS, windows))
        pick = jnp.sum(jnp.where(hit, picks, 0), axis=1, keepdims=True)
        taper = jnp.broadcast_to(bank_ref[0:1, :], (ROWS, FREQ))
        for t in range(1, TAPERS):
            taper = jnp.where(pick == t, bank_ref[t : t + 1, :], taper)
        weight = taper * noise_ref[...]
        real = (weight * vis_ref[:, 0, :].astype(jnp.float32)).astype(jnp.bfloat16)
        imag = (weight * vis_ref[:, 1, :].astype(jnp.float32)).astype(jnp.bfloat16)
        left = jnp.concatenate(
            [jnp.concatenate([real, imag], axis=1), jnp.concatenate([imag, -real], axis=1)], axis=0
        )
        both = jnp.dot(left, table_ref[...], preferred_element_type=jnp.float32).astype(jnp.bfloat16)
        here = pl.ds(pl.multiple_of(step * ROWS, ROWS), ROWS)
        spectra_ref[here, :P_SIZE] = both[:ROWS]
        spectra_ref[here, P_SIZE:] = both[ROWS:]

    @pl.when(step == 0)
    def rank():
        count = row_ref.shape[1]
        groups = 2 * windows
        names = row_ref[...]
        match = jnp.broadcast_to(names, (groups, count)) == lax.broadcasted_iota(jnp.int32, (groups, count), 0)
        first = lax.broadcasted_iota(jnp.int32, (count, count), 0)
        second = lax.broadcasted_iota(jnp.int32, (count, count), 1)
        before = jnp.where(first < second, 1.0, 0.0).astype(jnp.bfloat16)
        member = jnp.where(match, 1.0, 0.0)
        earlier = jnp.dot(member.astype(jnp.bfloat16), before, preferred_element_type=jnp.float32)
        order = jnp.sum(member * earlier, axis=0, keepdims=True).astype(jnp.int32)
        upper = lax.axis_index("win") * 2 >= lax.axis_size("win")
        shifted = jnp.where(names >= windows, names - windows, names + windows)
        ordered = jnp.where(upper, names, shifted)
        if paired(windows):
            mine = (lax.axis_index("win") * lax.axis_size("band") + lax.axis_index("band")) % (windows // 2)
            ordered = jnp.where(ordered < windows, ordered, ordered ^ (2 * mine))
        split = ((ordered & 1) * (windows // 2) + ordered // 2) * capacity
        slot_ref[...] = jnp.where(ordered < windows, split, ordered * capacity) + order

    @pl.when((step >= steps) & (step < steps + quarter))
    def first():
        first_ref[...] = placed_rows((step - steps) * SLOTS, slot_ref, spectra_ref)

    @pl.when(step >= steps + quarter)
    def second():
        second_ref[...] = placed_rows((step - steps) * SLOTS, slot_ref, spectra_ref)


def placed_rows(first, slot_ref, spectra_ref):
    count = slot_ref.shape[1]
    wanted = lax.broadcasted_iota(jnp.int32, (SLOTS, count), 0) + first
    choose = jnp.where(jnp.broadcast_to(slot_ref[...], (SLOTS, count)) == wanted, 1.0, 0.0).astype(jnp.bfloat16)
    return jnp.dot(choose, spectra_ref[...], preferred_element_type=jnp.float32).astype(jnp.bfloat16)


def near_kernel(offset, slot_ref, spectra_ref, out_ref):
    out_ref[...] = placed_rows(offset + pl.program_id(0) * SLOTS, slot_ref, spectra_ref)


def near_slots(slots, spectra, offset):
    count, spectral = spectra.shape
    return pl.pallas_call(
        functools.partial(near_kernel, offset),
        grid=(offset // SLOTS,),
        out_shape=jax.ShapeDtypeStruct((offset, spectral), jnp.bfloat16),
        in_specs=[pl.BlockSpec((1, count), lambda s: (0, 0)), pl.BlockSpec((count, spectral), lambda s: (0, 0))],
        out_specs=pl.BlockSpec((SLOTS, spectral), lambda s: (s, 0)),
        name="near",
    )(slots, spectra)


def near_parts_kernel(offset, slot_ref, spectra_ref, *out_refs):
    rows_each = out_refs[0].shape[0]
    per_step = SLOTS // rows_each
    for c in range(len(out_refs) // per_step):
        rows = placed_rows(offset + c * SLOTS, slot_ref, spectra_ref)
        for t in range(per_step):
            out_refs[c * per_step + t][...] = rows[rows_each * t : rows_each * (t + 1)]


def near_parts(slots, spectra, offset, half):
    spectral = spectra.shape[1]
    return pl.pallas_call(
        functools.partial(near_parts_kernel, offset),
        out_shape=[jax.ShapeDtypeStruct((offset // half, spectral), jnp.bfloat16)] * half,
        name="near",
    )(slots, spectra)


def far_slots(vis, inv_noise, assign, taper_bank, taper_pick, windows, capacity):
    pair_count = assign.shape[0]
    steps = pair_count // ROWS
    slots = windows * capacity // 2
    quarter = slots // SLOTS
    last = steps - 1
    names = assign[None, :]

    def early(step):
        return jnp.minimum(step, last)

    return pl.pallas_call(
        functools.partial(front_kernel, steps, capacity, quarter),
        grid=(steps + 2 * quarter,),
        out_shape=[
            jax.ShapeDtypeStruct((slots, 2 * P_SIZE), jnp.bfloat16),
            jax.ShapeDtypeStruct((slots, 2 * P_SIZE), jnp.bfloat16),
            jax.ShapeDtypeStruct((pair_count, 2 * P_SIZE), jnp.bfloat16),
            jax.ShapeDtypeStruct((1, pair_count), jnp.int32),
        ],
        in_specs=[
            pl.BlockSpec((ROWS, 2, FREQ), lambda s: (early(s), 0, 0)),
            pl.BlockSpec((ROWS, FREQ), lambda s: (early(s), 0)),
            pl.BlockSpec((1, ROWS), lambda s: (0, early(s))),
            pl.BlockSpec((1, pair_count), lambda s: (0, 0)),
            pl.BlockSpec((1, windows), lambda s: (0, 0)),
            pl.BlockSpec((TAPERS, FREQ), lambda s: (0, 0)),
            pl.BlockSpec((FREQ, P_SIZE), lambda s: (0, 0)),
        ],
        out_specs=[
            pl.BlockSpec((SLOTS, 2 * P_SIZE), lambda s: (jnp.clip(s - steps, 0, quarter - 1), 0)),
            pl.BlockSpec((SLOTS, 2 * P_SIZE), lambda s: (jnp.maximum(s - steps - quarter, 0), 0)),
            pl.BlockSpec((pair_count, 2 * P_SIZE), lambda s: (0, 0)),
            pl.BlockSpec((1, pair_count), lambda s: (0, 0)),
        ],
        scratch_shapes=[pltpu.VMEM((2 * FREQ, P_SIZE), jnp.bfloat16)],
        compiler_params=pltpu.CompilerParams(dimension_semantics=("arbitrary",)),
        name="front",
    )(vis, inv_noise, names, names, taper_pick[None, :], taper_bank, delay_parts())


def packed_moments(rows):
    sources, capacity, spectral = rows.shape
    size = spectral // 2
    rows = rows.reshape(sources * capacity, spectral)
    first, second = rows[:, :size], rows[:, size:]
    mixed = cross(second, rows)
    real = cross(first, first) + mixed[:, size:]
    imag = mixed[:, :size] - mixed[:, :size].T
    r = lax.broadcasted_iota(jnp.int32, (size, size), 0)
    c = lax.broadcasted_iota(jnp.int32, (size, size), 1)
    packed = jnp.where(r <= c, real, imag)
    return packed, jnp.sum(jnp.where(r == c, real, 0.0), axis=0, keepdims=True)


def far_kernel(rows_ref, packed_ref, power_ref):
    packed, power = packed_moments(rows_ref[...])
    packed_ref[0] = packed.astype(jnp.bfloat16)
    power_ref[0] = power


def near_moment_kernel(rows_ref, first_ref, second_ref, packed_ref, trace_ref, power_ref):
    packed, power = packed_moments(rows_ref[...])
    packed_ref[0] = packed
    total = power + jnp.where(pl.program_id(0) == 0, first_ref[0], second_ref[0])

    @pl.when(pl.program_id(0) == 0)
    def keep():
        power_ref[...] = total

    @pl.when(pl.program_id(0) == 1)
    def combine():
        both = 0.5 * power_ref[...] * total
        lanes = both[:, :LANE]
        for t in range(1, both.shape[1] // LANE):
            lanes = lanes + both[:, LANE * t : LANE * (t + 1)]
        trace_ref[...] = jnp.broadcast_to(lanes, trace_ref.shape)


def power_kernel(rows_ref, power_ref):
    sources, capacity, spectral = rows_ref.shape
    size = spectral // 2
    rows = rows_ref[...].reshape(sources * capacity, spectral).astype(jnp.float32)
    total = jnp.sum(rows * rows, axis=0, keepdims=True)
    power_ref[0] = total[:, :size] + total[:, size:]


def far_power(incoming):
    size = incoming.shape[2] // 2
    return pl.pallas_call(
        power_kernel, out_shape=jax.ShapeDtypeStruct((1, 1, size), jnp.float32), name="far_power"
    )(incoming)


def paired_moment_kernel(count, *refs):
    parts, (first_ref, second_ref, packed_ref, trace_ref) = refs[:count], refs[count:]
    capacity = parts[0].shape[0] // 2
    powers = []
    for g, far_ref in enumerate((first_ref, second_ref)):
        rows = jnp.concatenate([part[capacity * g : capacity * (g + 1), :] for part in parts], axis=0)
        packed, power = packed_moments(rows[None])
        packed_ref[g] = packed
        powers.append(power + far_ref[0])
    both = 0.5 * powers[0] * powers[1]
    lanes = both[:, :LANE]
    for t in range(1, both.shape[1] // LANE):
        lanes = lanes + both[:, LANE * t : LANE * (t + 1)]
    trace_ref[...] = jnp.broadcast_to(lanes, trace_ref.shape)


def paired_moments(parts, first, second, windows):
    size = parts[0].shape[1] // 2
    return pl.pallas_call(
        functools.partial(paired_moment_kernel, len(parts)),
        out_shape=[
            jax.ShapeDtypeStruct((2, size, size), jnp.float32),
            jax.ShapeDtypeStruct((windows, 1, LANE), jnp.float32),
        ],
        name="near_moments",
    )(*parts, first, second)


def far_moments(incoming):
    _, _, spectral = incoming.shape
    size = spectral // 2
    return pl.pallas_call(
        far_kernel,
        out_shape=[
            jax.ShapeDtypeStruct((1, size, size), jnp.bfloat16),
            jax.ShapeDtypeStruct((1, 1, size), jnp.float32),
        ],
        name="far_moments",
    )(incoming)


def near_moments(incoming, first, second, windows):
    sources, both, spectral = incoming.shape
    size = spectral // 2
    power = pl.BlockSpec((1, 1, size), lambda g: (0, 0, 0))
    return pl.pallas_call(
        near_moment_kernel,
        grid=(2,),
        out_shape=[
            jax.ShapeDtypeStruct((2, size, size), jnp.float32),
            jax.ShapeDtypeStruct((windows, 1, LANE), jnp.float32),
        ],
        in_specs=[pl.BlockSpec((sources, both // 2, spectral), lambda g: (0, g, 0)), power, power],
        out_specs=[
            pl.BlockSpec((1, size, size), lambda g: (g, 0, 0)),
            pl.BlockSpec((windows, 1, LANE), lambda g: (0, 0, 0)),
        ],
        scratch_shapes=[pltpu.VMEM((1, size), jnp.float32)],
        compiler_params=pltpu.CompilerParams(dimension_semantics=("arbitrary",)),
        name="near_moments",
    )(incoming, first, second)


def local(vis, inv_noise, assign, taper_bank, taper_pick):
    win_size = lax.axis_size("win")
    band_size = lax.axis_size("band")
    windows = win_size * band_size
    capacity = assign.shape[0] // windows
    spectral = 2 * P_SIZE
    half = windows // 2
    groups = [list(range(half)), list(range(half, windows))]
    mirror = [(i, (i + half) % windows) for i in range(windows)]
    everywhere = ("win", "band")

    def gather_half(rows):
        rows = rows.reshape(half, rows.shape[0] // half, spectral)
        return lax.all_to_all(
            rows, everywhere, split_axis=0, concat_axis=0, axis_index_groups=groups, tiled=True
        )

    *fars, spectra, slots = far_slots(vis, inv_noise, assign, taper_bank, taper_pick, windows, capacity)
    if paired(windows):
        parts = list(near_parts(slots, spectra, windows * capacity, half))
    else:
        near = near_slots(slots, spectra, windows * capacity)
    received, powers = [], []
    for g, far in enumerate(fars):
        far = gather_half(far)
        packed, power = far_moments(far)
        if paired(windows) and g == 0:
            power = far_power(far)
        powers.append(lax.ppermute(power, everywhere, mirror))
        received.append(lax.ppermute(packed, everywhere, mirror))
    if paired(windows):
        for k in range(1, half):
            parts[k] = lax.ppermute(parts[k], everywhere, [(i, i ^ k) for i in range(windows)])
        near, traces = paired_moments(parts, *powers, windows)
    else:
        near = gather_half(near)
        near, traces = near_moments(near, *powers, windows)
    traces = lax.all_to_all(traces, everywhere, split_axis=0, concat_axis=0, tiled=True)
    return factor_rows(traces, near, *received)[None]


def solution(mesh):
    in_specs = (
        P(("win", "band"), None, None),
        P(("win", "band"), None),
        P(("win", "band")),
        P(),
        P(),
    )
    out_specs = P(("win", "band"), None, None)
    return jax.shard_map(local, mesh=mesh, in_specs=in_specs, out_specs=out_specs, check_vma=False)
```
